32 devices in a mesh: gx: 4 (over x, core), gy: 2 (over y), gz: 4 (over z).
Axes of the slice: x: 2, y: 2, z: 4, core: 2. Of those that a mesh axis runs over, the one named last changes fastest.
Arguments:
- output_grad: bfloat16 [32768, 1024], P(('gx', 'gy', 'gz')), may hold values from -6 to 6
- entries: int32 [32768, 32], P(('gx', 'gy', 'gz')), may hold values from 0 to 511, as said below
- weights: bfloat16 [32768, 32], P(('gx', 'gy', 'gz')), may hold values from 0.0099487305 to 0.099609375
- hot_blocks: int32 [32, 4], P(('gx', 'gy', 'gz')), may hold values from -1 to 15, as said below
- block_counts: int32 [32], P(('gx', 'gy', 'gz')), may hold values from 2 to 4, as said below
- param: float32 [4, 4, 128, 1024], P('gx', 'gz', 'gy'), may hold values from -6 to 6
- first_moment: float32 [4, 4, 128, 1024], P('gx', 'gz', 'gy'), may hold values from -4 to 4
- second_moment: float32 [4, 4, 128, 1024], P('gx', 'gz', 'gy'), may hold values from 0.05 to 1
Outputs:
- new_param: float32 [4, 4, 128, 1024], P('gx', 'gz', 'gy')
- new_first: float32 [4, 4, 128, 1024], P('gx', 'gz', 'gy')
- new_second: float32 [4, 4, 128, 1024], P('gx', 'gz', 'gy')
The draws below stay inside these ranges and needn't reach their ends.
Inputs may be any that keep to these rules, and one draw needn't show every extreme that they name: `hot_blocks`: row d lists device d's hot blocks (block b is rows b * 128 to b * 128 + 127 of the table laid out as 2048 rows) in its first block_counts[d] slots and -1 in the others. The listed blocks of one row differ pairwise modulo 4. Among the devices that differ only in their gz index, some value modulo 4 is listed by every one of them. `block_counts`: among the devices that differ only in their gz index, at least one uses all 4 slots. `entries`: an entry e of a token of device d names a used slot: e // 128 < block_counts[d].
All inputs are finite; a program needn't handle non-finite values.
Results may differ from the reference program's by a relative error of at most 0.00034.
Values sent between devices are 32-bit elements; how exact they have to be, the bound alone decides.
A program may use at most 128 MiB of HBM per device.

```python
import math
import jax
import jax.numpy as jnp
from jax import lax

D = 1024
BLOCK = 128
KNN = 32
TOK_DEV = 1024
HOT = 4
NBLK = 16
TOKENS = 32768
N_GX = 4
N_GZ = 4
DEVICES = 32


def shuffled_row(row_key):
    return jax.random.permutation(row_key, HOT).astype(jnp.int32)


def hot_lists(key):
    keys = jax.random.split(jax.random.fold_in(key, 5), 8)
    line_count = DEVICES // N_GZ
    device = jnp.arange(DEVICES, dtype=jnp.int32)
    line = device // N_GZ
    position = device % N_GZ
    counts = jax.random.randint(keys[0], (DEVICES,), HOT // 2, HOT + 1, dtype=jnp.int32)
    full_member = jax.random.randint(keys[1], (line_count,), 0, N_GZ, dtype=jnp.int32)
    counts = jnp.where(position == full_member[line], HOT, counts).astype(jnp.int32)
    orders = jax.vmap(shuffled_row)(jax.random.split(keys[2], DEVICES))
    common = jax.random.randint(keys[3], (line_count,), 0, N_GZ, dtype=jnp.int32)[line]
    target = jax.random.randint(keys[4], (DEVICES,), 0, counts, dtype=jnp.int32)
    slot_index = jnp.arange(HOT, dtype=jnp.int32)
    where_now = jnp.argmax(orders == common[:, None], axis=1).astype(jnp.int32)
    at_target = jnp.take_along_axis(orders, target[:, None], axis=1)
    orders = jnp.where(slot_index[None, :] == target[:, None], common[:, None], jnp.where(slot_index[None, :] == where_now[:, None], at_target, orders))
    first_pick = jax.random.randint(keys[5], (DEVICES, HOT), 0, N_GX, dtype=jnp.int32)
    second_pick = jax.random.randint(keys[6], (DEVICES, HOT), 0, N_GX, dtype=jnp.int32)
    offset = jax.random.randint(keys[7], (), 0, N_GX, dtype=jnp.int32)
    column = (jnp.minimum(first_pick, second_pick) + offset) % N_GX
    blocks = jnp.where(slot_index[None, :] < counts[:, None], column * N_GZ + orders, -1)
    return (blocks.astype(jnp.int32), counts)


def draw_hot_blocks(key, part):
    return hot_lists(key)[0]


def draw_block_counts(key, part):
    return hot_lists(key)[1]


def draw_entries(key, part):
    counts = hot_lists(key)[1]
    slot_key, row_key = jax.random.split(jax.random.fold_in(key, 11))
    owner = jnp.arange(TOKENS, dtype=jnp.int32) // TOK_DEV
    slot_pick = jax.random.randint(slot_key, (TOKENS, KNN), 0, counts[owner][:, None], dtype=jnp.int32)
    row_pick = jax.random.randint(row_key, (TOKENS, KNN), 0, BLOCK, dtype=jnp.int32)
    return (slot_pick * BLOCK + row_pick).astype(jnp.int32)


def block_scale(key, dims, cuts, smallest, top_value):
    def one(dim, shards_of):
        draws = jax.random.uniform(jax.random.fold_in(jax.random.fold_in(key, 6), dim), (shards_of,), jnp.float32, smallest / len(cuts), top_value / len(cuts))
        return jnp.repeat(jnp.exp(draws), dims[dim] // shards_of).reshape((-1,) + (1,) * (len(dims) - dim - 1))

    gain = one(*cuts[0])
    for cut in cuts[1:]:
        gain = gain * one(*cut)
    return gain


def bell_draw(rng, extent, scale, limit, cuts=(), kind=jnp.bfloat16):
    result = jax.random.normal(rng, extent, jnp.float32) * scale
    if len(cuts) > 0:
        result = block_scale(rng, extent, cuts, -0.22, 0.18) * result
    return jnp.clip(result, min=-limit, max=limit).astype(kind)


def setup_inputs(seed: int = 0) -> dict:
    arg_keys = jax.random.split(jax.random.key(seed), 9)
    output_grad = bell_draw(arg_keys[0], (TOKENS, D), 1.0, 6.0, ((0, 32),))
    entries = draw_entries(jax.random.fold_in(arg_keys[8], 71), 0)
    weights = jnp.clip(0.0099487305 + 0.089660645 * jax.random.uniform(arg_keys[2], (TOKENS, KNN), jnp.float32) ** block_scale(arg_keys[2], (TOKENS, KNN), ((0, 32),), -0.2, 0.2), 0.0099487305, 0.099609375).astype(jnp.bfloat16)
    hot_blocks = draw_hot_blocks(jax.random.fold_in(arg_keys[8], 71), 0)
    block_counts = draw_block_counts(jax.random.fold_in(arg_keys[8], 71), 0)
    param = bell_draw(arg_keys[5], (N_GX, N_GZ, BLOCK, D), 1.0, 6.0, ((0, 4), (1, 4), (2, 2)), jnp.float32)
    first_moment = bell_draw(arg_keys[6], (N_GX, N_GZ, BLOCK, D), 0.5, 4.0, ((0, 4), (1, 4), (2, 2)), jnp.float32)
    second_moment = jnp.clip(jnp.exp(math.log(1.0) - 2.9957323 * jax.random.uniform(arg_keys[7], (N_GX, N_GZ, BLOCK, D), jnp.float32) ** block_scale(arg_keys[7], (N_GX, N_GZ, BLOCK, D), ((0, 4), (1, 4), (2, 2)), -0.2, 0.2)), 0.05, 1.0)
    return dict(output_grad=output_grad, entries=entries, weights=weights, hot_blocks=hot_blocks, block_counts=block_counts, param=param, first_moment=first_moment, second_moment=second_moment)


first_decay = 0.9
second_decay = 0.99
learning_rate = 0.01
adam_epsilon = 1e-08
first_debias = 1.0 / (1.0 - 0.9 ** 10)
second_debias = 1.0 / (1.0 - 0.99 ** 10)

def reference(output_grad, entries, weights, hot_blocks, block_counts, param, first_moment, second_moment):
    slot_index = jnp.arange(HOT, dtype=jnp.int32)
    token_index = jnp.arange(TOK_DEV, dtype=jnp.int32)[:, None]

    def device_step(device, totals):
        start = (device * TOK_DEV).astype(jnp.int32)
        grads = lax.dynamic_slice_in_dim(output_grad, start, TOK_DEV, 0)
        picks = lax.dynamic_slice_in_dim(entries, start, TOK_DEV, 0).astype(jnp.int32)
        scales = lax.dynamic_slice_in_dim(weights, start, TOK_DEV, 0)
        listed = lax.dynamic_index_in_dim(hot_blocks, device, 0, keepdims=False).astype(jnp.int32)
        used = lax.dynamic_index_in_dim(block_counts, device, 0, keepdims=False).astype(jnp.int32)
        flat_index = (picks * TOK_DEV + token_index).reshape(-1)
        spread = jnp.zeros((HOT * BLOCK * TOK_DEV,), jnp.float32).at[flat_index].add(scales.astype(jnp.float32).reshape(-1))
        spread = spread.reshape(HOT * BLOCK, TOK_DEV).astype(jnp.bfloat16)
        partial_value = jnp.dot(spread, grads, preferred_element_type=jnp.float32)
        usable = (slot_index < used) & (listed >= 0)
        target = jnp.where(usable, listed, NBLK).astype(jnp.int32)
        return totals.at[target].add(partial_value.reshape(HOT, BLOCK, D), mode='drop')
    totals = lax.fori_loop(0, DEVICES, device_step, jnp.zeros((NBLK, BLOCK, D), jnp.float32))
    gradient = totals.reshape(N_GX, N_GZ, BLOCK, D)
    new_first = first_decay * first_moment + (1.0 - first_decay) * gradient
    new_second = second_decay * second_moment + (1.0 - second_decay) * gradient * gradient
    new_param = param - learning_rate * (new_first * first_debias) / (jnp.sqrt(new_second * second_debias) + adam_epsilon)
    return (new_param, new_first, new_second)
```

```python
import functools

import jax
import jax.numpy as jnp
from jax import lax
from jax.experimental import pallas as pl
from jax.experimental.pallas import tpu as pltpu
from jax.sharding import PartitionSpec as P

first_decay = 0.9
second_decay = 0.99
learning_rate = 0.01
adam_epsilon = 1e-08
first_debias = 1.0 / (1.0 - 0.9**10)
second_debias = 1.0 / (1.0 - 0.99**10)

MESH = pl.DeviceIdType.MESH
PIECES = 2
AHEAD = 2
LANES = 128


def adam_update(gradient, param, first_moment, second_moment):
    new_first = first_decay * first_moment + (1.0 - first_decay) * gradient
    new_second = second_decay * second_moment + (1.0 - second_decay) * gradient * gradient
    new_param = param - learning_rate * (new_first * first_debias) / (
        jnp.sqrt(new_second * second_debias) + adam_epsilon
    )
    return (new_param, new_first, new_second)


def kernel(
    sizes,
    hot_ref, count_ref, entries_ref, weights_ref, grad_hbm,
    out_ref,
    grad, code_t, weight_t, spread, partial,
    label_own, label_recv,
    a_recv, b1_send, b1_recv, b2_send, b2_recv, merged, c_recv,
    grad_sem, la_send, la_recv, sa_send, sa_recv, s1_send, s1_recv, s2_send, s2_recv,
    sc_send, sc_recv,
):
    gx_size, gy_size, gz_size, block, slots = sizes
    halves = gx_size // 2
    tokens, width = grad_hbm.shape
    piece = width // PIECES
    rows = block // gy_size
    knn = entries_ref.shape[0]
    count = gz_size * PIECES
    gx, gy, gz = lax.axis_index("gx"), lax.axis_index("gy"), lax.axis_index("gz")
    high, low = gx // 2, gx % 2

    def gy_peer(j):
        return {"gy": (gy + j) % gy_size}

    def high_peer(j):
        return {"gx": ((high + j) % halves) * 2 + low}

    pair_peer = {"gx": high * 2 + 1 - low}
    peers = [gy_peer(j) for j in range(1, gy_size)]
    peers += [pair_peer]
    peers += [high_peer(j) for j in range(1, halves)]
    peers += [{"gz": (gz + j) % gz_size} for j in range(1, gz_size)]

    barrier = pltpu.get_barrier_semaphore()
    for peer in peers:
        pl.semaphore_signal(barrier, inc=1, device_id=peer, device_id_type=MESH)
    load = pltpu.make_async_copy(grad_hbm, grad, grad_sem)
    load.start()

    def bucket_at(p):
        if p == gz_size - 1:
            return gz
        upper = (2 * gz) // gz_size
        down = gz_size - 1 - p
        from_top = down - (gz - down + gz_size) // gz_size
        from_bottom = p + (p - gz + gz_size) // gz_size
        return (1 - upper) * from_top + upper * from_bottom

    bases, columns, buckets = [], [], []
    for s in range(slots):
        listed = hot_ref[0, s]
        usable = (s < count_ref[0]) & (listed >= 0)
        safe = jnp.maximum(listed, 0)
        bucket = safe % gz_size
        bases.append(jnp.where(usable, bucket * block, -(2**20)))
        columns.append(jnp.where(usable, safe // gz_size, -1))
        buckets.append(jnp.where(usable, bucket, -1))
    labels = []
    for p in range(gz_size):
        b = bucket_at(p)
        label = jnp.int32(-1)
        for s in range(slots):
            label = jnp.where(buckets[s] == b, columns[s], label)
        labels.append(label)
        label_own[p] = jnp.full((8, LANES), label, jnp.int32)

    entry = entries_ref[...]
    slot, row = entry // block, entry % block
    code = jnp.full(entry.shape, -1, jnp.int32)
    for s in range(slots):
        code = jnp.where(slot == s, bases[s] + row, code)
    code_t[...] = code
    weight_t[...] = weights_ref[...].astype(jnp.float32)

    row_index = lax.broadcasted_iota(jnp.int32, (block, LANES), 0)

    def make_spread(p):
        first_row = bucket_at(p) * block

        def lane_tile(j, carry):
            at = pl.ds(pl.multiple_of(j * LANES, LANES), LANES)
            total = jnp.zeros((block, LANES), jnp.float32)
            for k in range(knn):
                target = code_t[pl.ds(k, 1), at] - first_row
                weight = weight_t[pl.ds(k, 1), at]
                total = total + jnp.where(row_index == target, weight, 0.0)
            spread[:, at] = total.astype(jnp.bfloat16)
            return carry

        lax.fori_loop(0, tokens // LANES, lane_tile, 0)

    sent = []

    def remote(src, dst, send_sem, recv_sem, peer):
        return pltpu.make_async_remote_copy(
            src_ref=src, dst_ref=dst, send_sem=send_sem, recv_sem=recv_sem,
            device_id=peer, device_id_type=MESH,
        )

    def launch(copy):
        copy.start()
        sent.append(copy)

    a_copies, b1_copies, b2_copies = {}, {}, {}

    def stage_a(i):
        p, f = i // PIECES, i % PIECES
        if f == 0:
            make_spread(p)
        if i == 0:
            load.wait()
        partial[i] = jnp.dot(
            spread[...], grad[:, f * piece:(f + 1) * piece], preferred_element_type=jnp.float32
        )
        if i == 0:
            pl.semaphore_wait(barrier, len(peers))
            for j in range(1, gy_size):
                copy = remote(label_own, label_recv.at[j - 1], la_send.at[j - 1],
                              la_recv.at[j - 1], gy_peer(j))
                launch(copy)
                a_copies["label", j] = copy
        for j in range(1, gy_size):
            to = (gy + j) % gy_size
            copy = remote(
                partial.at[i, pl.ds(pl.multiple_of(to * rows, rows), rows), :],
                a_recv.at[i, j - 1], sa_send.at[i, j - 1], sa_recv.at[i, j - 1], gy_peer(j),
            )
            launch(copy)
            a_copies[i, j] = copy

    def column_sum(i, column):
        p = i // PIECES
        mine = partial[i, pl.ds(pl.multiple_of(gy * rows, rows), rows), :]
        total = jnp.where(label_own[p, 0:1, 0:1] == column, mine, 0.0)
        for j in range(1, gy_size):
            total = total + jnp.where(
                label_recv[j - 1, p, 0:1, 0:1] == column, a_recv[i, j - 1], 0.0
            )
        return total

    def stage_b1(i):
        for j in range(1, gy_size):
            if i == 0:
                a_copies["label", j].wait_recv()
            a_copies[i, j].wait_recv()
        for t in range(halves):
            b1_send[i, t] = column_sum(i, ((high + t) % halves) * 2 + 1 - low)
        copy = remote(b1_send.at[i], b1_recv.at[i], s1_send.at[i], s1_recv.at[i], pair_peer)
        launch(copy)
        b1_copies[i] = copy

    def stage_b2(i):
        b1_copies[i].wait_recv()
        for t in range(1, halves):
            b2_send[i, t - 1] = column_sum(i, ((high + t) % halves) * 2 + low) + b1_recv[i, t]
            copy = remote(b2_send.at[i, t - 1], b2_recv.at[i, t - 1], s2_send.at[i, t - 1],
                          s2_recv.at[i, t - 1], high_peer(t))
            launch(copy)
            b2_copies[i, t] = copy
        merged[i] = column_sum(i, high * 2 + low) + b1_recv[i, 0]

    def stage_c(i):
        p, f = i // PIECES, i % PIECES
        for t in range(1, halves):
            b2_copies[i, t].wait_recv()
        total = merged[i]
        for t in range(1, halves):
            total = total + b2_recv[i, t - 1]
        if p < gz_size - 1:
            merged[i] = total
            launch(remote(merged.at[i], c_recv.at[gz, f], sc_send.at[i], sc_recv.at[gz, f],
                          {"gz": bucket_at(p)}))
            return
        for j in range(1, gz_size):
            source = (gz + j) % gz_size
            remote(merged.at[i], c_recv.at[source, f], sc_send.at[i], sc_recv.at[source, f],
                   {"gz": source}).wait_recv()
            total = total + c_recv[source, f]
        out_ref[:, f * piece:(f + 1) * piece] = total

    for i in range(count + AHEAD + 1):
        if 0 <= i - AHEAD < count:
            stage_b1(i - AHEAD)
        if i < count:
            stage_a(i)
        if 0 <= i - AHEAD < count:
            stage_b2(i - AHEAD)
        if 0 <= i - AHEAD - 1 < count:
            stage_c(i - AHEAD - 1)
    for copy in sent:
        copy.wait_send()


def shards(
    output_grad, entries, weights, hot_blocks, block_counts, param, first_moment, second_moment
):
    gx_size, gy_size, gz_size = (lax.axis_size(a) for a in ("gx", "gy", "gz"))
    slots = hot_blocks.shape[1]
    tokens, width = output_grad.shape
    rows = param.shape[2]
    block = rows * gy_size
    knn = entries.shape[1]
    piece = width // PIECES
    count = gz_size * PIECES
    halves = gx_size // 2
    f32 = jnp.float32
    dma = pltpu.SemaphoreType.DMA
    gradient = pl.pallas_call(
        functools.partial(kernel, (gx_size, gy_size, gz_size, block, slots)),
        out_shape=jax.ShapeDtypeStruct((rows, width), f32),
        in_specs=[
            pl.BlockSpec(memory_space=pltpu.SMEM),
            pl.BlockSpec(memory_space=pltpu.SMEM),
            pl.BlockSpec(memory_space=pltpu.VMEM),
            pl.BlockSpec(memory_space=pltpu.VMEM),
            pl.BlockSpec(memory_space=pl.ANY),
        ],
        out_specs=pl.BlockSpec(memory_space=pltpu.VMEM),
        scratch_shapes=[
            pltpu.VMEM((tokens, width), jnp.bfloat16),
            pltpu.VMEM((knn, tokens), jnp.int32),
            pltpu.VMEM((knn, tokens), f32),
            pltpu.VMEM((block, tokens), jnp.bfloat16),
            pltpu.VMEM((count, block, piece), f32),
            pltpu.VMEM((gz_size, 8, LANES), jnp.int32),
            pltpu.VMEM((gy_size - 1, gz_size, 8, LANES), jnp.int32),
            pltpu.VMEM((count, gy_size - 1, rows, piece), f32),
            pltpu.VMEM((count, halves, rows, piece), f32),
            pltpu.VMEM((count, halves, rows, piece), f32),
            pltpu.VMEM((count, halves - 1, rows, piece), f32),
            pltpu.VMEM((count, halves - 1, rows, piece), f32),
            pltpu.VMEM((count, rows, piece), f32),
            pltpu.VMEM((gz_size, PIECES, rows, piece), f32),
            dma,
            dma((gy_size - 1,)),
            dma((gy_size - 1,)),
            dma((count, gy_size - 1)),
            dma((count, gy_size - 1)),
            dma((count,)),
            dma((count,)),
            dma((count, halves - 1)),
            dma((count, halves - 1)),
            dma((count,)),
            dma((gz_size, PIECES)),
        ],
        compiler_params=pltpu.CompilerParams(
            collective_id=0, has_side_effects=True, vmem_limit_bytes=56 * 1024 * 1024
        ),
        cost_estimate=pl.CostEstimate(
            flops=2 * tokens * width * block * gz_size, bytes_accessed=tokens * width * 2,
            transcendentals=0,
        ),
    )(hot_blocks, block_counts, entries.T, weights.T, output_grad)
    return adam_update(gradient.reshape(param.shape), param, first_moment, second_moment)


def solution(mesh):
    tokens = P(("gx", "gy", "gz"), None)
    table = P("gx", "gz", "gy", None)
    placed = (tokens, tokens, tokens, tokens, P(("gx", "gy", "gz")), table, table, table)
    return jax.shard_map(
        shards, mesh=mesh, in_specs=placed, out_specs=(table, table, table), check_vma=False
    )
```

```python
import functools

import jax
import jax.numpy as jnp
from jax import lax
from jax.experimental import pallas as pl
from jax.experimental.pallas import tpu as pltpu
from jax.sharding import PartitionSpec as P

first_decay = 0.9
second_decay = 0.99
learning_rate = 0.01
adam_epsilon = 1e-08
first_debias = 1.0 / (1.0 - 0.9**10)
second_debias = 1.0 / (1.0 - 0.99**10)

MESH = pl.DeviceIdType.MESH
PIECES = 2
AHEAD = 3
LATE = PIECES
PAIR_LAG = 0
HIGH_LAG = 3
LANES = 128


def adam_update(gradient, param, first_moment, second_moment):
    new_first = first_decay * first_moment + (1.0 - first_decay) * gradient
    new_second = second_decay * second_moment + (1.0 - second_decay) * gradient * gradient
    new_param = param - learning_rate * (new_first * first_debias) / (
        jnp.sqrt(new_second * second_debias) + adam_epsilon
    )
    return (new_param, new_first, new_second)


def kernel(
    sizes,
    hot_ref, count_ref, entries_ref, weights_ref, grad_hbm,
    out_ref,
    grad, code_t, weight_t, spread, partial,
    label_own, label_recv,
    a_recv, b1_send, b1_recv, b2_send, b2_recv, merged, c_recv,
    grad_sem, la_send, la_recv, sa_send, sa_recv, s1_send, s1_recv, s2_send, s2_recv,
    sc_send, sc_recv,
):
    gx_size, gy_size, gz_size, block, slots = sizes
    halves = gx_size // 2
    tokens, width = grad_hbm.shape
    piece = width // PIECES
    rows = block // gy_size
    knn = entries_ref.shape[0]
    count = gz_size * PIECES
    gx, gy, gz = lax.axis_index("gx"), lax.axis_index("gy"), lax.axis_index("gz")
    high, low = gx // 2, gx % 2

    def gy_peer(j):
        return {"gy": (gy + j) % gy_size}

    def high_peer(j):
        return {"gx": ((high + j) % halves) * 2 + low}

    pair_peer = {"gx": high * 2 + 1 - low}
    peers = [gy_peer(j) for j in range(1, gy_size)]
    peers += [pair_peer]
    peers += [high_peer(j) for j in range(1, halves)]
    peers += [{"gz": (gz + 1) % gz_size}, {"gz": (gz + gz_size - 1) % gz_size}]

    barrier = pltpu.get_barrier_semaphore()
    for peer in peers:
        pl.semaphore_signal(barrier, inc=1, device_id=peer, device_id_type=MESH)
    load = pltpu.make_async_copy(grad_hbm, grad, grad_sem)
    load.start()

    def bucket_at(p):
        if p == gz_size - 1:
            return gz
        upper = (2 * gz) // gz_size
        down = gz_size - 1 - p
        from_top = down - (gz - down + gz_size) // gz_size
        from_bottom = p + (p - gz + gz_size) // gz_size
        return (1 - upper) * from_top + upper * from_bottom

    bases, columns, buckets = [], [], []
    for s in range(slots):
        listed = hot_ref[0, s]
        usable = (s < count_ref[0]) & (listed >= 0)
        safe = jnp.maximum(listed, 0)
        bucket = safe % gz_size
        bases.append(jnp.where(usable, bucket * block, -(2**20)))
        columns.append(jnp.where(usable, safe // gz_size, -1))
        buckets.append(jnp.where(usable, bucket, -1))
    labels = []
    for p in range(gz_size):
        b = bucket_at(p)
        label = jnp.int32(-1)
        for s in range(slots):
            label = jnp.where(buckets[s] == b, columns[s], label)
        labels.append(label)
        label_own[p] = jnp.full((8, LANES), label, jnp.int32)

    entry = entries_ref[...]
    slot, row = entry // block, entry % block
    code = jnp.full(entry.shape, -1, jnp.int32)
    for s in range(slots):
        code = jnp.where(slot == s, bases[s] + row, code)
    code_t[...] = code
    weight_t[...] = weights_ref[...].astype(jnp.float32)

    row_index = lax.broadcasted_iota(jnp.int32, (block, LANES), 0)

    def make_spread(p):
        first_row = bucket_at(p) * block

        def lane_tile(j, carry):
            at = pl.ds(pl.multiple_of(j * LANES, LANES), LANES)
            total = jnp.zeros((block, LANES), jnp.float32)
            for k in range(knn):
                target = code_t[pl.ds(k, 1), at] - first_row
                weight = weight_t[pl.ds(k, 1), at]
                total = total + jnp.where(row_index == target, weight, 0.0)
            spread[:, at] = total.astype(jnp.bfloat16)
            return carry

        lax.fori_loop(0, tokens // LANES, lane_tile, 0)

    sent = []

    def remote(src, dst, send_sem, recv_sem, peer):
        return pltpu.make_async_remote_copy(
            src_ref=src, dst_ref=dst, send_sem=send_sem, recv_sem=recv_sem,
            device_id=peer, device_id_type=MESH,
        )

    def launch(copy):
        copy.start()
        sent.append(copy)

    a_copies, b1_copies, b2_copies = {}, {}, {}

    def stage_a(i):
        p, f = i // PIECES, i % PIECES
        if f == 0:
            make_spread(p)
        if i == 0:
            load.wait()
        partial[i] = jnp.dot(
            spread[...], grad[:, f * piece:(f + 1) * piece], preferred_element_type=jnp.float32
        )
        if i == 0:
            pl.semaphore_wait(barrier, len(peers))
            for j in range(1, gy_size):
                copy = remote(label_own, label_recv.at[j - 1], la_send.at[j - 1],
                              la_recv.at[j - 1], gy_peer(j))
                launch(copy)
                a_copies["label", j] = copy
        for j in range(1, gy_size):
            to = (gy + j) % gy_size
            copy = remote(
                partial.at[i, pl.ds(pl.multiple_of(to * rows, rows), rows), :],
                a_recv.at[i, j - 1], sa_send.at[i, j - 1], sa_recv.at[i, j - 1], gy_peer(j),
            )
            launch(copy)
            a_copies[i, j] = copy

    def column_sum(i, column):
        p = i // PIECES
        mine = partial[i, pl.ds(pl.multiple_of(gy * rows, rows), rows), :]
        total = jnp.where(label_own[p, 0:1, 0:1] == column, mine, 0.0)
        for j in range(1, gy_size):
            total = total + jnp.where(
                label_recv[j - 1, p, 0:1, 0:1] == column, a_recv[i, j - 1], 0.0
            )
        return total

    def stage_b1(i):
        for j in range(1, gy_size):
            if i == 0:
                a_copies["label", j].wait_recv()
            a_copies[i, j].wait_recv()
        for t in range(halves):
            b1_send[i, t] = column_sum(i, ((high + t) % halves) * 2 + 1 - low)
        copy = remote(b1_send.at[i], b1_recv.at[i], s1_send.at[i], s1_recv.at[i], pair_peer)
        launch(copy)
        b1_copies[i] = copy

    def stage_b2(i):
        b1_copies[i].wait_recv()
        for t in range(1, halves):
            b2_send[i, t - 1] = column_sum(i, ((high + t) % halves) * 2 + low) + b1_recv[i, t]
            copy = remote(b2_send.at[i, t - 1], b2_recv.at[i, t - 1], s2_send.at[i, t - 1],
                          s2_recv.at[i, t - 1], high_peer(t))
            launch(copy)
            b2_copies[i, t] = copy
        merged[i] = column_sum(i, high * 2 + low) + b1_recv[i, 0]

    from_below = (gz + gz_size - 1) // gz_size
    from_above = (2 * gz_size - 2 - gz) // gz_size

    def line_copy(i):
        p, f = i // PIECES, i % PIECES
        bucket = bucket_at(p)
        up = (bucket - gz + gz_size) // gz_size
        copy = remote(merged.at[i], c_recv.at[up, bucket, f], sc_send.at[i],
                      sc_recv.at[up, bucket, f], {"gz": gz + 2 * up - 1})
        relays = up * from_below + (1 - up) * from_above
        return copy, relays, up, bucket, f

    def stage_c(i):
        for t in range(1, halves):
            b2_copies[i, t].wait_recv()
        total = merged[i]
        for t in range(1, halves):
            total = total + b2_recv[i, t - 1]
        merged[i] = total
        if i // PIECES < gz_size - 1:
            copy, relays = line_copy(i)[:2]

            @pl.when(relays == 0)
            def _():
                copy.start()

    def add_arrived(i, direction, bucket, f):
        remote(merged.at[i], c_recv.at[direction, bucket, f], sc_send.at[i],
               sc_recv.at[direction, bucket, f], {"gz": (gz + 1) % gz_size}).wait_recv()
        merged[i] = merged[i] + c_recv[direction, bucket, f]

    def stage_relay(i):
        f = i % PIECES
        if i // PIECES < gz_size - 1:
            copy, relays, up, bucket, _ = line_copy(i)

            @pl.when(relays == 1)
            def _():
                add_arrived(i, up, bucket, f)
                copy.start()

            return

        @pl.when(from_below == 1)
        def _():
            add_arrived(i, 1, gz, f)

        @pl.when(from_above == 1)
        def _():
            add_arrived(i, 0, gz, f)

        out_ref[:, f * piece:(f + 1) * piece] = merged[i]

    def relay_step(i):
        return i + AHEAD + HIGH_LAG + (LATE if i // PIECES < gz_size - 2 else 0)

    for step in range(count + AHEAD + HIGH_LAG + LATE):
        i = step - AHEAD
        if 0 <= i < count:
            stage_b1(i)
        if step < count:
            stage_a(step)
        if 0 <= i - PAIR_LAG < count:
            stage_b2(i - PAIR_LAG)
        if 0 <= i - HIGH_LAG < count:
            stage_c(i - HIGH_LAG)
        for r in range(count):
            if relay_step(r) == step:
                stage_relay(r)
    for copy in sent:
        copy.wait_send()
    for i in range(count - PIECES):
        line_copy(i)[0].wait_send()


def shards(
    output_grad, entries, weights, hot_blocks, block_counts, param, first_moment, second_moment
):
    gx_size, gy_size, gz_size = (lax.axis_size(a) for a in ("gx", "gy", "gz"))
    slots = hot_blocks.shape[1]
    tokens, width = output_grad.shape
    rows = param.shape[2]
    block = rows * gy_size
    knn = entries.shape[1]
    piece = width // PIECES
    count = gz_size * PIECES
    halves = gx_size // 2
    f32 = jnp.float32
    dma = pltpu.SemaphoreType.DMA
    gradient = pl.pallas_call(
        functools.partial(kernel, (gx_size, gy_size, gz_size, block, slots)),
        out_shape=jax.ShapeDtypeStruct((rows, width), f32),
        in_specs=[
            pl.BlockSpec(memory_space=pltpu.SMEM),
            pl.BlockSpec(memory_space=pltpu.SMEM),
            pl.BlockSpec(memory_space=pltpu.VMEM),
            pl.BlockSpec(memory_space=pltpu.VMEM),
            pl.BlockSpec(memory_space=pl.ANY),
        ],
        out_specs=pl.BlockSpec(memory_space=pltpu.VMEM),
        scratch_shapes=[
            pltpu.VMEM((tokens, width), jnp.bfloat16),
            pltpu.VMEM((knn, tokens), jnp.int32),
            pltpu.VMEM((knn, tokens), f32),
            pltpu.VMEM((block, tokens), jnp.bfloat16),
            pltpu.VMEM((count, block, piece), f32),
            pltpu.VMEM((gz_size, 8, LANES), jnp.int32),
            pltpu.VMEM((gy_size - 1, gz_size, 8, LANES), jnp.int32),
            pltpu.VMEM((count, gy_size - 1, rows, piece), f32),
            pltpu.VMEM((count, halves, rows, piece), f32),
            pltpu.VMEM((count, halves, rows, piece), f32),
            pltpu.VMEM((count, halves - 1, rows, piece), f32),
            pltpu.VMEM((count, halves - 1, rows, piece), f32),
            pltpu.VMEM((count, rows, piece), f32),
            pltpu.VMEM((2, gz_size, PIECES, rows, piece), f32),
            dma,
            dma((gy_size - 1,)),
            dma((gy_size - 1,)),
            dma((count, gy_size - 1)),
            dma((count, gy_size - 1)),
            dma((count,)),
            dma((count,)),
            dma((count, halves - 1)),
            dma((count, halves - 1)),
            dma((count,)),
            dma((2, gz_size, PIECES)),
        ],
        compiler_params=pltpu.CompilerParams(
            collective_id=0, has_side_effects=True, vmem_limit_bytes=56 * 1024 * 1024
        ),
        cost_estimate=pl.CostEstimate(
            flops=2 * tokens * width * block * gz_size, bytes_accessed=tokens * width * 2,
            transcendentals=0,
        ),
    )(hot_blocks, block_counts, entries.T, weights.T, output_grad)
    return adam_update(gradient.reshape(param.shape), param, first_moment, second_moment)


def solution(mesh):
    tokens = P(("gx", "gy", "gz"), None)
    table = P("gx", "gz", "gy", None)
    placed = (tokens, tokens, tokens, tokens, P(("gx", "gy", "gz")), table, table, table)
    return jax.shard_map(
        shards, mesh=mesh, in_specs=placed, out_specs=(table, table, table), check_vma=False
    )
```
